32 devices in a mesh: expert: 16 (over z, y, x), replica: 2 (over core).
Axes of the slice: x: 2, y: 2, z: 4, core: 2. Of those that a mesh axis runs over, the one named last changes fastest.
Arguments:
- tokens: bfloat16 [16384, 1024], P(('expert', 'replica')), may hold values from -6 to 6
- expert_id: int32 [16384, 1], P(('expert', 'replica')), may hold values from 0 to 15; in each aligned block of 512 rows (0 to 511, 512 to 1023, ...) at most 64 rows name the same one
- router_prob: float32 [16384], P(('expert', 'replica')), may hold values from 0.1 to 1
- keep_mask: int32 [16, 32, 2048], P('expert'), may hold values 0 or 1
- w_in: bfloat16 [16, 1024, 2048], P('expert'), may hold values from -0.1875 to 0.1875
- w_out: bfloat16 [16, 2048, 1024], P('expert'), may hold values from -0.125 to 0.125
- cotangent: bfloat16 [16384, 1024], P(('expert', 'replica')), may hold values from -0.59765625 to 0.59765625
Outputs:
- mixed: bfloat16 [16384, 1024], P(('expert', 'replica'))
- grad_in: float32 [16, 1024, 2048], P('expert', 'replica')
- grad_out: float32 [16, 2048, 1024], P('expert', 'replica')
The draws below stay inside these ranges and needn't reach their ends.
Inputs may be any that keep to these rules, and one draw needn't show every extreme that they name: `expert_id`: among the 512 tokens of one device no expert is chosen more than 64 times; on some devices one expert is chosen exactly 64 times.
All inputs are finite; a program needn't handle non-finite values. No bound on the sum of `keep_mask` on one device may be relied on, other than what follows from the above.
Results may differ from the reference program's by a relative error of at most 0.0057.
Values may be sent and summed in bfloat16 or wider, within the bound.
A program may use at most 128 MiB of HBM per device.

```python
import math
import jax
import jax.numpy as jnp
import numpy as np
from jax import lax

D = 1024
FF = 2048
TOK_DEV = 512
EXPERTS = 16
SOURCES = 32
TOKENS = 16384
CAP = 64


def set_ends(result, key, smallest, largest):
    longest = result.shape.index(max(result.shape))
    spots = []
    for shift in (0, 1):
        where = [jax.random.randint(jax.random.fold_in(key, axis), (), 0, length) for axis, length in enumerate(result.shape)]
        where[longest] = (where[longest] + shift) % result.shape[longest]
        spots.append(tuple(where))
    return result.at[spots[0]].set(smallest).at[spots[1]].set(largest)


def level_of(own_key, dims, shards, low, high):
    def one(axis_at, parts):
        steps = jax.random.uniform(jax.random.fold_in(jax.random.fold_in(own_key, 6), axis_at), (parts,), jnp.float32, low / len(shards), high / len(shards))
        return jnp.repeat(jnp.exp(steps), dims[axis_at] // parts).reshape((-1,) + (1,) * (len(dims) - axis_at - 1))

    gain = one(*shards[0])
    for cut in shards[1:]:
        gain = gain * one(*cut)
    return gain


def deal_out(own_key, own, number, rows, count, top, limit, skew):
    ranking = jax.random.permutation(own_key, count)
    packed, common = portions_of(count, rows * top, limit, skew, True), portions_of(count, rows * top, limit, skew, False)
    places = jnp.arange(count)

    def named(sizes, rotation):
        used = int((sizes > 0).sum())
        fixed = max(1, used // 4)
        shifted = fixed + (places - fixed + rotation * (used - fixed)) % max(1, count - fixed)
        return jnp.zeros((count,), jnp.int32).at[ranking[jnp.where(places < fixed, places, shifted)]].set(jnp.asarray(sizes, jnp.int32))

    sizes = jnp.where(number % 4 == 0, named(packed, number // 4), named(common, number - number // 4 - 1))
    mixed = jax.random.permutation(jax.random.fold_in(own, 3), count)
    giver, taker = mixed[0:count // 2 * 2:2], mixed[1:count // 2 * 2:2]
    room = jnp.minimum(sizes[giver] - 1, limit - sizes[taker]) // 2
    room = jnp.where((giver == ranking[0]) | (taker == ranking[0]) | (sizes[taker] == 0), 0, jnp.maximum(room, 0))
    shifted = jax.random.randint(jax.random.fold_in(own, 4), (count // 2,), 0, 1 << 20) % (room + 1)
    sizes = sizes.at[giver].add(-shifted).at[taker].add(shifted)
    items = jnp.searchsorted(jnp.cumsum(sizes), jnp.arange(rows * top), side="right").astype(jnp.int32)
    listing = items.reshape(top, rows).T
    listing = listing[jax.random.permutation(jax.random.fold_in(own, 1), rows)]
    rotation = jax.random.randint(jax.random.fold_in(own, 2), (rows, 1), 0, top)
    return jnp.take_along_axis(listing, (jnp.arange(top)[None, :] + rotation) % top, axis=1)


def portions_of(number_of, total, reach, skew, full):
    weights = [(1 << 20) // math.isqrt(grade ** skew) + 1 for grade in range(1, number_of + 1)]
    largest = reach if full else min(reach, max(-(-total // number_of), total * weights[0] // sum(weights)))
    least = 1 if total - largest >= number_of - 1 else 0
    holding, surplus = [largest] + [least] * (number_of - 1), total - largest - least * (number_of - 1)
    while surplus > 0:
        candidates = [i for i in range(1, number_of) if holding[i] < largest] or [i for i in range(1, number_of) if holding[i] < reach]
        whole, remaining = sum([weights[i] for i in candidates]), surplus
        for i in candidates:
            extra = min(reach - holding[i], max(1, remaining * weights[i] // whole), surplus)
            holding[i] = holding[i] + extra
            surplus = surplus - extra
    return np.array(holding)


def centred(own_key, dims, deviation, most, pieces=(), kind=jnp.bfloat16):
    loudness = level_of(own_key, dims, pieces, -0.22, 0.18) if pieces else 1.0
    drawn = jax.random.normal(own_key, dims, jnp.float32) * deviation * loudness
    return jnp.minimum(jnp.maximum(drawn, -most), most).astype(kind)


def setup_inputs(seed: int = 0) -> dict:
    splits = jax.random.split(jax.random.key(seed), 8)
    tokens = centred(splits[0], (TOKENS, D), 1.0, 6.0, ((0, 32),))
    expert_id_keys = jax.random.split(jax.random.fold_in(splits[1], 1), TOKENS // TOK_DEV)
    expert_id_turns = jax.random.permutation(jax.random.fold_in(splits[1], 3), TOKENS // TOK_DEV)
    expert_id = jax.vmap(lambda own, number: deal_out(jax.random.fold_in(splits[1], 2), own, number, TOK_DEV, EXPERTS, 1, CAP, 2))(expert_id_keys, expert_id_turns).reshape((TOKENS, 1))
    router_prob = jnp.clip(0.1 + 0.9 * jax.random.uniform(splits[2], (TOKENS,), jnp.float32) ** level_of(splits[2], (TOKENS,), ((0, 32),), -0.2, 0.2), 0.1, 1.0)
    keep_mask = set_ends((jax.random.randint(splits[3], (EXPERTS, SOURCES, FF), 0, 4) < 3).astype(jnp.int32), jax.random.fold_in(splits[3], 1), 0, 1)
    w_in = centred(splits[4], (EXPERTS, D, FF), D ** -0.5, 0.1875, ((0, 16),))
    w_out = centred(splits[5], (EXPERTS, FF, D), FF ** -0.5, 0.125, ((0, 16),))
    cotangent = centred(splits[6], (TOKENS, D), 0.1, 0.59765625, ((0, 32),))
    return dict(tokens=tokens, expert_id=expert_id, router_prob=router_prob, keep_mask=keep_mask, w_in=w_in, w_out=w_out, cotangent=cotangent)


KEEP_SCALE = 4.0 / 3.0


def gelu_parts(pre):
    inner = 0.7978845608 * (pre + 0.044715 * pre * pre * pre)
    tanh_v = jnp.tanh(inner)
    value = 0.5 * pre * (1.0 + tanh_v)
    slope = 0.5 * (1.0 + tanh_v) + 0.5 * pre * (1.0 - tanh_v * tanh_v) * 0.7978845608 * (1.0 + 3.0 * 0.044715 * pre * pre)
    return value, slope


def reference(tokens, expert_id, router_prob, keep_mask, w_in, w_out, cotangent):
    ids = expert_id[:, 0].astype(jnp.int32)
    per = ids.reshape(SOURCES, TOK_DEV)
    onehot = (per[:, :, None] == jnp.arange(EXPERTS, dtype=jnp.int32)[None, None, :]).astype(jnp.int32)
    rank = (jnp.sum(jnp.cumsum(onehot, axis=1) * onehot, axis=2) - 1).reshape(TOKENS).astype(jnp.int32)
    source = (jnp.arange(TOKENS, dtype=jnp.int32) // TOK_DEV).astype(jnp.int32)
    place = (ids * (SOURCES * CAP) + source * CAP + rank).astype(jnp.int32)
    table = jnp.full((EXPERTS * SOURCES * CAP,), TOKENS, jnp.int32).at[place].set(jnp.arange(TOKENS, dtype=jnp.int32))
    table = table.reshape(EXPERTS, SOURCES * CAP)
    gated = (router_prob[:, None] * cotangent.astype(jnp.float32)).astype(jnp.bfloat16)
    x_pad = jnp.concatenate([tokens, jnp.zeros((1, D), tokens.dtype)], axis=0)
    g_pad = jnp.concatenate([gated, jnp.zeros((1, D), gated.dtype)], axis=0)

    def one_expert(args):
        index_row, weight_in, weight_out, keep_rows = args
        rows_x = x_pad[index_row]
        rows_g = g_pad[index_row]
        keep_scale = jnp.repeat(keep_rows.astype(jnp.float32) * KEEP_SCALE, CAP, axis=0)
        pre = jnp.dot(rows_x, weight_in, preferred_element_type=jnp.float32)
        value, slope = gelu_parts(pre)
        hidden = (value * keep_scale).astype(jnp.bfloat16)
        out = jnp.dot(hidden, weight_out, preferred_element_type=jnp.float32).astype(jnp.bfloat16)
        g_out = jnp.dot(hidden.T, rows_g, preferred_element_type=jnp.float32)
        dhidden = jnp.dot(rows_g, weight_out.T, preferred_element_type=jnp.float32)
        dpre = (dhidden * keep_scale * slope).astype(jnp.bfloat16)
        g_in = jnp.dot(rows_x.T, dpre, preferred_element_type=jnp.float32)
        return out, g_in, g_out

    outs, grad_in, grad_out = lax.map(one_expert, (table, w_in, w_out, keep_mask))
    flat = outs.reshape(EXPERTS * SOURCES * CAP, D)
    expert_out = flat[place]
    mixed = (router_prob[:, None] * expert_out.astype(jnp.float32)).astype(jnp.bfloat16)
    return mixed, grad_in, grad_out
```

```python
import functools

import jax
import jax.numpy as jnp
from jax import lax
from jax.experimental import pallas as pl
from jax.experimental.pallas import tpu as pltpu
from jax.sharding import PartitionSpec as P

KEEP_SCALE = 4.0 / 3.0
MESH = pl.DeviceIdType.MESH


def gelu_parts(pre):
    inner = 0.7978845608 * (pre + 0.044715 * pre * pre * pre)
    tanh_v = jnp.tanh(inner)
    value = 0.5 * pre * (1.0 + tanh_v)
    slope = 0.5 * (1.0 + tanh_v) + 0.5 * pre * (1.0 - tanh_v * tanh_v) * 0.7978845608 * (
        1.0 + 3.0 * 0.044715 * pre * pre
    )
    return (value, slope)


def tile_of(size, most):
    return size if size <= most else most


def each(low, high, step):
    def run(i, carry):
        step(i)
        return carry

    lax.fori_loop(low, high, run, 0)


def kernel(
    n, shifts,
    ids, prob, tokens, cotangent, keep, w_in, w_out,
    mixed, grad_in, grad_out,
    own_x, own_g, keep_raw, keep_rows, slot, columns_of,
    sent, sent_grad, back,
    weight_in, weight_out, rows_x, rows_g, rows_o, hidden, factor, dpre,
    give_out, give_in, came_out, came_in,
    load_sem, own_sem, x_send, x_recv, g_send, g_recv, o_send, o_recv, pair_send, pair_recv,
):
    me = lax.axis_index("expert")
    core = lax.axis_index("replica")
    other = 1 - core
    group = n // shifts
    plane = me // group
    spot = lax.rem(me, group)
    cap, width = rows_x.shape[1:]
    ff = weight_in.shape[1]
    rows = group * cap
    tile = tile_of(ff, 512)
    wide = tile_of(width, 256)
    count = own_x.shape[0]
    total = factor.at[pl.ds(0, count), pl.ds(0, width)]

    def load(i):
        source, target = (
            (tokens, own_x), (cotangent, own_g), (keep, keep_raw), (w_in, weight_in), (w_out, weight_out)
        )[i]
        return pltpu.make_async_copy(source, target, load_sem.at[i])

    for i in range(5):
        load(i).start()

    def ahead(shift, turn):
        return lax.rem(plane + shift, shifts) * group + lax.rem(spot + turn, group)

    def behind(shift, turn):
        return lax.rem(plane - shift + shifts, shifts) * group + lax.rem(spot - turn + group, group)

    def x_copy(shift, turn):
        k = shift * group + turn
        return pltpu.make_async_remote_copy(
            src_ref=sent.at[k], dst_ref=rows_x.at[k], send_sem=x_send.at[k],
            recv_sem=x_recv.at[k], device_id=(ahead(shift, turn), core), device_id_type=MESH,
        )

    def g_copy(shift, turn):
        k = shift * group + turn
        return pltpu.make_async_remote_copy(
            src_ref=sent_grad.at[k], dst_ref=rows_g.at[k], send_sem=g_send.at[k],
            recv_sem=g_recv.at[k], device_id=(ahead(shift, turn), core), device_id_type=MESH,
        )

    def o_copy(shift, turn):
        k = shift * group + turn
        return pltpu.make_async_remote_copy(
            src_ref=rows_o.at[k], dst_ref=back.at[k], send_sem=o_send.at[k],
            recv_sem=o_recv.at[k], device_id=(behind(shift, turn), core), device_id_type=MESH,
        )

    def own_copy(i):
        source, target = (
            (sent.at[0], rows_x.at[0]), (sent_grad.at[0], rows_g.at[0]), (rows_o.at[0], back.at[0])
        )[i]
        return pltpu.make_async_copy(source, target, own_sem.at[i])

    def pair_copy(i):
        source, target = ((give_out, came_out), (give_in, came_in))[i]
        return pltpu.make_async_remote_copy(
            src_ref=source, dst_ref=target, send_sem=pair_send.at[i],
            recv_sem=pair_recv.at[i], device_id=(me, other), device_id_type=MESH,
        )

    def blocks(shift, step):
        def one(turn):
            @pl.when(shift * group + turn > 0)
            def _():
                step(shift, turn)

        each(0, group, one)

    barrier = pltpu.get_barrier_semaphore()

    def greet(shift, turn):
        pl.semaphore_signal(barrier, inc=1, device_id=(ahead(shift, turn), core), device_id_type=MESH)

    each(0, shifts, lambda shift: blocks(shift, greet))
    pl.semaphore_signal(barrier, inc=1, device_id=(me, other), device_id_type=MESH)

    low = plane * 2 < shifts
    even = lax.rem(plane, 2) == 0

    def send_order(i):
        return jnp.where(low, lax.rem(i + 1, shifts), lax.rem(shifts - 1 - i + shifts, shifts))

    def near_first(i, sign):
        first = jnp.where(even, shifts - 1, 1)
        last = (plane + 3) // 2
        place = jnp.where(i == 0, 0, jnp.where(i == 1, first, jnp.where(i == 3, last, 6 - first - last)))
        if shifts != 4:
            place = i
        return place if sign > 0 else lax.rem(shifts - place, shifts)

    expert_rows = lax.broadcasted_iota(jnp.int32, (n, count), 0)
    hot = jnp.where(expert_rows == ids[...], 1.0, 0.0)
    before = lax.broadcasted_iota(jnp.int32, (count, count), 0) <= lax.broadcasted_iota(
        jnp.int32, (count, count), 1)
    counted = jnp.dot(
        hot.astype(jnp.bfloat16), jnp.where(before, 1.0, 0.0).astype(jnp.bfloat16),
        preferred_element_type=jnp.float32,
    )
    rank = jnp.sum(hot * counted, axis=0, keepdims=True) - 1.0
    place_of = ids[...] * cap + rank.astype(jnp.int32)
    slot[...] = place_of
    pair = lax.broadcasted_iota(jnp.int32, (128, count), 0) == 0
    columns_of[...] = jnp.transpose(jnp.where(pair, place_of.astype(jnp.float32), prob[...]))

    def dispatch(values, slots, shift):
        shape = (group, cap, count)
        turn = lax.broadcasted_iota(jnp.int32, shape, 0) + spot
        turn = jnp.where(turn >= group, turn - group, turn)
        place = (lax.rem(plane + shift, shifts) * group + turn) * cap + lax.broadcasted_iota(jnp.int32, shape, 1)
        chosen = jnp.where(place == slot[...][None], 1.0, 0.0).astype(jnp.bfloat16)
        filled = jnp.dot(
            chosen.reshape(rows, count), values[...], preferred_element_type=jnp.float32
        )
        slots[pl.ds(shift * group, group)] = filled.astype(jnp.bfloat16).reshape(group, cap, width)

    def start(copy):
        return lambda shift, turn: copy(shift, turn).start()

    load(0).wait()
    dispatch(own_x, sent, send_order(0))
    pl.semaphore_wait(barrier, n)

    def send_x(i):
        dispatch(own_x, sent, send_order(i))
        blocks(send_order(i - 1), start(x_copy))

    each(1, shifts, send_x)
    load(1).wait()
    own_g[...] = (columns_of[:, 1:2] * own_g[...].astype(jnp.float32)).astype(jnp.bfloat16)
    blocks(send_order(shifts - 1), start(x_copy))
    own_copy(0).start()

    def send_g(i):
        dispatch(own_g, sent_grad, send_order(i))

        @pl.when(i > 0)
        def _():
            blocks(send_order(i - 1), start(g_copy))

    each(0, shifts, send_g)
    load(2).wait()

    def keep_row(k):
        source = behind(k // group, lax.rem(k, group)) * 2 + core
        keep_rows[k] = keep_raw[pl.ds(source, 1), :].astype(jnp.float32) * KEEP_SCALE

    each(0, n, keep_row)
    blocks(send_order(shifts - 1), start(g_copy))
    own_copy(1).start()
    own_copy(0).wait()
    own_copy(1).wait()
    load(3).wait()
    load(4).wait()

    def forward(i):
        shift = near_first(i, 1)
        first = shift * group
        span = pl.ds(pl.multiple_of(first * cap, rows), rows)
        blocks(shift, lambda s, t: x_copy(s, t).wait_recv())

        def project(j):
            columns = pl.ds(pl.multiple_of(j * tile, tile), tile)
            block = rows_x[pl.ds(first, group)].reshape(rows, width)
            pre = jnp.dot(block, weight_in[:, columns], preferred_element_type=jnp.float32)
            value, slope = gelu_parts(pre)
            scale = keep_rows[pl.ds(first, group), :, columns]
            value = value.reshape(group, cap, tile) * scale
            slope = slope.reshape(group, cap, tile) * scale
            hidden[pl.ds(first, group), :, columns] = value.astype(jnp.bfloat16)
            factor[span, columns] = slope.reshape(rows, tile)

        each(0, ff // tile, project)

        def output(j):
            columns = pl.ds(pl.multiple_of(j * wide, wide), wide)
            block = hidden[pl.ds(first, group)].reshape(rows, ff)
            out = jnp.dot(block, weight_out[:, columns], preferred_element_type=jnp.float32)
            rows_o[pl.ds(first, group), :, columns] = out.astype(jnp.bfloat16).reshape(group, cap, wide)

        each(0, width // wide, output)
        blocks(shift, start(o_copy))

        @pl.when(shift == 0)
        def _():
            own_copy(2).start()

    each(0, shifts, forward)

    def backward(i):
        shift = near_first(i, 1)
        first = shift * group
        span = pl.ds(pl.multiple_of(first * cap, rows), rows)
        blocks(shift, lambda s, t: g_copy(s, t).wait_recv())

        def pull(j):
            columns = pl.ds(pl.multiple_of(j * tile, tile), tile)
            block = rows_g[pl.ds(first, group)].reshape(rows, width)
            dhidden = lax.dot_general(
                block, weight_out[columns, :], (((1,), (1,)), ((), ())),
                preferred_element_type=jnp.float32,
            )
            dhidden = (dhidden * factor[span, columns]).astype(jnp.bfloat16)
            dpre[pl.ds(first, group), :, columns] = dhidden.reshape(group, cap, tile)

        each(0, ff // tile, pull)

    each(0, shifts, backward)

    def product(left, right, first, j, part):
        columns = pl.ds(pl.multiple_of(first + j * part, part), part)
        return lax.dot_general(
            left[:, :, columns].reshape(n * cap, part), right[...].reshape(n * cap, right.shape[2]),
            (((0,), (0,)), ((), ())), preferred_element_type=jnp.float32,
        )

    def gradient(left, right, give, came, result):
        half = give.shape[0]
        part = tile_of(half, 256)

        def theirs(j):
            give[pl.ds(pl.multiple_of(j * part, part), part), :] = product(
                left, right, other * half, j, part).astype(jnp.bfloat16)

        def mine(j):
            band = pl.ds(pl.multiple_of(j * part, part), part)
            result[band, :] = came[band, :].astype(jnp.float32) + product(left, right, core * half, j, part)

        return functools.partial(each, 0, half // part, theirs), functools.partial(each, 0, half // part, mine)

    theirs_out, mine_out = gradient(hidden, rows_g, give_out, came_out, grad_out)
    theirs_in, mine_in = gradient(rows_x, dpre, give_in, came_in, grad_in)
    theirs_out()
    pair_copy(0).start()
    theirs_in()
    pair_copy(1).start()
    pair_copy(0).wait_recv()
    mine_out()
    pair_copy(1).wait_recv()
    mine_in()
    pair_copy(0).wait_send()
    own_copy(2).wait()

    def chosen_of(shift):
        lane = lax.broadcasted_iota(jnp.int32, (count, rows), 1)
        turn = lane // cap + spot
        turn = jnp.where(turn >= group, turn - group, turn)
        place = (lax.rem(plane + shift, shifts) * group + turn) * cap + lax.rem(lane, cap)
        return jnp.where(place == columns_of[:, 0:1].astype(jnp.int32), 1.0, 0.0).astype(jnp.bfloat16)

    def part_of(chosen, shift, columns):
        return jnp.dot(
            chosen, back[pl.ds(shift * group, group), :, columns].reshape(rows, wide),
            preferred_element_type=jnp.float32,
        )

    def combine(i):
        shift = near_first(i, -1)
        chosen = chosen_of(shift)
        blocks(shift, lambda s, t: o_copy(s, t).wait_recv())
        for j in range(width // wide):
            columns = pl.ds(j * wide, wide)
            added = part_of(chosen, shift, columns)

            @pl.when(i == 0)
            def _():
                total[:, columns] = added

            @pl.when(i > 0)
            def _():
                total[:, columns] += added

    each(0, shifts - 1, combine)

    def finish(shift, turn):
        x_copy(shift, turn).wait_send()
        g_copy(shift, turn).wait_send()

    each(0, shifts, lambda shift: blocks(shift, finish))
    pair_copy(1).wait_send()
    shift = near_first(shifts - 1, -1)
    chosen = chosen_of(shift)
    blocks(shift, lambda s, t: o_copy(s, t).wait_recv())
    for j in range(width // wide):
        columns = pl.ds(j * wide, wide)
        added = part_of(chosen, shift, columns)
        mixed[:, columns] = (columns_of[:, 1:2] * (total[:, columns] + added)).astype(jnp.bfloat16)
    each(0, shifts, lambda shift: blocks(shift, lambda s, t: o_copy(s, t).wait_send()))


def exchange(n, cap, ids, prob, tokens, cotangent, keep, w_in, w_out):
    count, width = tokens.shape
    ff = w_in.shape[1]
    shifts = 4 if n % 4 == 0 else 1
    dma = pltpu.SemaphoreType.DMA
    f32, bf16 = jnp.float32, jnp.bfloat16
    whole = pl.BlockSpec(memory_space=pl.ANY)
    near = pl.BlockSpec(memory_space=pltpu.VMEM)
    flops = 10 * n * cap * width * ff
    return pl.pallas_call(
        functools.partial(kernel, n, shifts),
        out_shape=(
            pltpu.VMEM((count, width), bf16),
            pltpu.VMEM((width // 2, ff), f32),
            pltpu.VMEM((ff // 2, width), f32),
        ),
        in_specs=[near] * 2 + [whole] * 5,
        out_specs=(near, near, near),
        scratch_shapes=[
            pltpu.VMEM((count, width), bf16),
            pltpu.VMEM((count, width), bf16),
            pltpu.VMEM(keep.shape, jnp.int32),
            pltpu.VMEM((n, 1, ff), f32),
            pltpu.VMEM((1, count), jnp.int32),
            pltpu.VMEM((count, 128), f32),
            pltpu.VMEM((n, cap, width), bf16),
            pltpu.VMEM((n, cap, width), bf16),
            pltpu.VMEM((n, cap, width), bf16),
            pltpu.VMEM((width, ff), bf16),
            pltpu.VMEM((ff, width), bf16),
            pltpu.VMEM((n, cap, width), bf16),
            pltpu.VMEM((n, cap, width), bf16),
            pltpu.VMEM((n, cap, width), bf16),
            pltpu.VMEM((n, cap, ff), bf16),
            pltpu.VMEM((n * cap, ff), f32),
            pltpu.VMEM((n, cap, ff), bf16),
            pltpu.VMEM((ff // 2, width), bf16),
            pltpu.VMEM((width // 2, ff), bf16),
            pltpu.VMEM((ff // 2, width), bf16),
            pltpu.VMEM((width // 2, ff), bf16),
            dma((5,)), dma((3,)), dma((n,)), dma((n,)), dma((n,)), dma((n,)), dma((n,)), dma((n,)),
            dma((2,)), dma((2,)),
        ],
        cost_estimate=pl.CostEstimate(flops=flops, bytes_accessed=40 << 20, transcendentals=n * cap * ff),
        compiler_params=pltpu.CompilerParams(
            collective_id=0, has_side_effects=True, vmem_limit_bytes=52 << 20
        ),
    )(ids, prob, tokens, cotangent, keep, w_in, w_out)


def shards(tokens, expert_id, router_prob, keep_mask, w_in, w_out, cotangent):
    count = tokens.shape[0]
    n = lax.axis_size("expert")
    mixed, grad_in, grad_out = exchange(
        n, 2 * count // n, expert_id.reshape(1, count), router_prob.reshape(1, count),
        tokens, cotangent, keep_mask[0], w_in[0], w_out[0],
    )
    return (mixed, grad_in[None], grad_out[None])


def solution(mesh):
    in_specs = (
        P(("expert", "replica"), None),
        P(("expert", "replica"), None),
        P(("expert", "replica")),
        P("expert", None, None),
        P("expert", None, None),
        P("expert", None, None),
        P(("expert", "replica"), None),
    )
    out_specs = (
        P(("expert", "replica"), None),
        P("expert", "replica", None),
        P("expert", "replica", None),
    )
    return jax.shard_map(shards, mesh=mesh, in_specs=in_specs, out_specs=out_specs, check_vma=False)
```

```python
import functools

import jax
import jax.numpy as jnp
from jax import lax
from jax.experimental import pallas as pl
from jax.experimental.pallas import tpu as pltpu
from jax.sharding import PartitionSpec as P

KEEP_SCALE = 4.0 / 3.0
MESH = pl.DeviceIdType.MESH


def gelu_parts(pre):
    inner = 0.7978845608 * (pre + 0.044715 * pre * pre * pre)
    tanh_v = jnp.tanh(inner)
    value = 0.5 * pre * (1.0 + tanh_v)
    slope = 0.5 * (1.0 + tanh_v) + 0.5 * pre * (1.0 - tanh_v * tanh_v) * 0.7978845608 * (
        1.0 + 3.0 * 0.044715 * pre * pre
    )
    return (value, slope)


def tile_of(size, most):
    return size if size <= most else most


def each(low, high, step):
    def run(i, carry):
        step(i)
        return carry

    lax.fori_loop(low, high, run, 0)


def kernel(
    n, shifts,
    ids_in, prob_in, tokens, cotangent, keep, w_in, w_out,
    mixed, grad_in, grad_out,
    ids, prob, own_x, own_g, keep_raw, keep_rows, slot, columns_of,
    sent, sent_grad, back,
    weight_in, weight_out, rows_x, rows_g, rows_o, hidden, factor, dpre,
    give_out, give_in, came_out, came_in,
    load_sem, own_sem, x_send, x_recv, g_send, g_recv, o_send, o_recv, pair_send, pair_recv,
):
    me = lax.axis_index("expert")
    core = lax.axis_index("replica")
    other = 1 - core
    group = n // shifts
    plane = me // group
    spot = lax.rem(me, group)
    cap, width = rows_x.shape[1:]
    ff = weight_in.shape[1]
    rows = group * cap
    tile = tile_of(ff, 512)
    wide = tile_of(width, 256)
    count = own_x.shape[0]
    total = factor.at[pl.ds(0, count), pl.ds(0, width)]

    def load(i):
        source, target = (
            (tokens, own_x), (cotangent, own_g), (keep, keep_raw), (w_in, weight_in), (w_out, weight_out),
            (ids_in, ids), (prob_in, prob),
        )[i]
        return pltpu.make_async_copy(source, target, load_sem.at[i])

    load(5).start()
    load(6).start()
    load(0).start()

    def ahead(shift, turn):
        return lax.rem(plane + shift, shifts) * group + lax.rem(spot + turn, group)

    def behind(shift, turn):
        return lax.rem(plane - shift + shifts, shifts) * group + lax.rem(spot - turn + group, group)

    def x_copy(shift, turn):
        k = shift * group + turn
        return pltpu.make_async_remote_copy(
            src_ref=sent.at[k], dst_ref=rows_x.at[k], send_sem=x_send.at[k],
            recv_sem=x_recv.at[k], device_id=(ahead(shift, turn), core), device_id_type=MESH,
        )

    def g_copy(shift, turn):
        k = shift * group + turn
        return pltpu.make_async_remote_copy(
            src_ref=sent_grad.at[k], dst_ref=rows_g.at[k], send_sem=g_send.at[k],
            recv_sem=g_recv.at[k], device_id=(ahead(shift, turn), core), device_id_type=MESH,
        )

    def o_copy(shift, turn):
        k = shift * group + turn
        return pltpu.make_async_remote_copy(
            src_ref=rows_o.at[k], dst_ref=back.at[k], send_sem=o_send.at[k],
            recv_sem=o_recv.at[k], device_id=(behind(shift, turn), core), device_id_type=MESH,
        )

    def own_copy(i):
        source, target = (
            (sent.at[0], rows_x.at[0]), (sent_grad.at[0], rows_g.at[0]), (rows_o.at[0], back.at[0])
        )[i]
        return pltpu.make_async_copy(source, target, own_sem.at[i])

    def pair_copy(i):
        source, target = ((give_out, came_out), (give_in, came_in))[i]
        return pltpu.make_async_remote_copy(
            src_ref=source, dst_ref=target, send_sem=pair_send.at[i],
            recv_sem=pair_recv.at[i], device_id=(me, other), device_id_type=MESH,
        )

    def blocks(shift, step):
        def one(turn):
            @pl.when(shift * group + turn > 0)
            def _():
                step(shift, turn)

        each(0, group, one)

    barrier = pltpu.get_barrier_semaphore()

    def greet(shift, turn):
        pl.semaphore_signal(barrier, inc=1, device_id=(ahead(shift, turn), core), device_id_type=MESH)

    each(0, shifts, lambda shift: blocks(shift, greet))
    pl.semaphore_signal(barrier, inc=1, device_id=(me, other), device_id_type=MESH)

    low = plane * 2 < shifts
    even = lax.rem(plane, 2) == 0

    def send_order(i):
        return jnp.where(low, lax.rem(i + 1, shifts), lax.rem(shifts - 1 - i + shifts, shifts))

    def near_first(i, sign):
        first = jnp.where(even, shifts - 1, 1)
        last = (plane + 3) // 2
        place = jnp.where(i == 0, 0, jnp.where(i == 1, first, jnp.where(i == 3, last, 6 - first - last)))
        if shifts != 4:
            place = i
        return place if sign > 0 else lax.rem(shifts - place, shifts)

    load(5).wait()
    load(6).wait()
    expert_rows = lax.broadcasted_iota(jnp.int32, (n, count), 0)
    hot = jnp.where(expert_rows == ids[...], 1.0, 0.0)
    before = lax.broadcasted_iota(jnp.int32, (count, count), 0) <= lax.broadcasted_iota(
        jnp.int32, (count, count), 1)
    counted = jnp.dot(
        hot.astype(jnp.bfloat16), jnp.where(before, 1.0, 0.0).astype(jnp.bfloat16),
        preferred_element_type=jnp.float32,
    )
    rank = jnp.sum(hot * counted, axis=0, keepdims=True) - 1.0
    place_of = ids[...] * cap + rank.astype(jnp.int32)
    slot[...] = place_of
    pair = lax.broadcasted_iota(jnp.int32, (128, count), 0) == 0
    columns_of[...] = jnp.transpose(jnp.where(pair, place_of.astype(jnp.float32), prob[...]))

    def dispatch(values, slots, shift):
        shape = (group, cap, count)
        turn = lax.broadcasted_iota(jnp.int32, shape, 0) + spot
        turn = jnp.where(turn >= group, turn - group, turn)
        place = (lax.rem(plane + shift, shifts) * group + turn) * cap + lax.broadcasted_iota(jnp.int32, shape, 1)
        chosen = jnp.where(place == slot[...][None], 1.0, 0.0).astype(jnp.bfloat16)
        filled = jnp.dot(
            chosen.reshape(rows, count), values[...], preferred_element_type=jnp.float32
        )
        slots[pl.ds(shift * group, group)] = filled.astype(jnp.bfloat16).reshape(group, cap, width)

    def start(copy):
        return lambda shift, turn: copy(shift, turn).start()

    load(0).wait()
    for i in range(1, 5):
        load(i).start()
    def send_x(i):
        dispatch(own_x, sent, send_order(i))

        @pl.when(i == 0)
        def _():
            pl.semaphore_wait(barrier, n)

        blocks(send_order(i), start(x_copy))

    each(0, shifts, send_x)
    own_copy(0).start()
    load(1).wait()
    own_g[...] = (columns_of[:, 1:2] * own_g[...].astype(jnp.float32)).astype(jnp.bfloat16)

    def send_g(i):
        dispatch(own_g, sent_grad, send_order(i))
        blocks(send_order(i), start(g_copy))

    each(0, shifts, send_g)
    own_copy(1).start()
    load(2).wait()

    def keep_row(k):
        source = behind(k // group, lax.rem(k, group)) * 2 + core
        keep_rows[k] = keep_raw[pl.ds(source, 1), :].astype(jnp.float32) * KEEP_SCALE

    each(0, n, keep_row)
    own_copy(0).wait()
    own_copy(1).wait()
    load(3).wait()
    load(4).wait()

    def forward(i):
        shift = near_first(i, 1)
        first = shift * group
        span = pl.ds(pl.multiple_of(first * cap, rows), rows)
        blocks(shift, lambda s, t: x_copy(s, t).wait_recv())

        def project(j):
            columns = pl.ds(pl.multiple_of(j * tile, tile), tile)
            block = rows_x[pl.ds(first, group)].reshape(rows, width)
            pre = jnp.dot(block, weight_in[:, columns], preferred_element_type=jnp.float32)
            value, slope = gelu_parts(pre)
            scale = keep_rows[pl.ds(first, group), :, columns]
            value = value.reshape(group, cap, tile) * scale
            slope = slope.reshape(group, cap, tile) * scale
            hidden[pl.ds(first, group), :, columns] = value.astype(jnp.bfloat16)
            factor[span, columns] = slope.reshape(rows, tile)

        each(0, ff // tile, project)

        def output(j):
            columns = pl.ds(pl.multiple_of(j * wide, wide), wide)
            block = hidden[pl.ds(first, group)].reshape(rows, ff)
            out = jnp.dot(block, weight_out[:, columns], preferred_element_type=jnp.float32)
            rows_o[pl.ds(first, group), :, columns] = out.astype(jnp.bfloat16).reshape(group, cap, wide)

        each(0, width // wide, output)

        @pl.when(i < shifts // 2)
        def _():
            blocks(shift, start(o_copy))

        @pl.when(shift == 0)
        def _():
            own_copy(2).start()

    each(0, shifts, forward)
    each(0, shifts - shifts // 2, lambda i: blocks(near_first(shifts - 1 - i, 1), start(o_copy)))

    def backward(i):
        shift = near_first(i, 1)
        first = shift * group
        span = pl.ds(pl.multiple_of(first * cap, rows), rows)
        blocks(shift, lambda s, t: g_copy(s, t).wait_recv())

        def pull(j):
            columns = pl.ds(pl.multiple_of(j * tile, tile), tile)
            block = rows_g[pl.ds(first, group)].reshape(rows, width)
            dhidden = lax.dot_general(
                block, weight_out[columns, :], (((1,), (1,)), ((), ())),
                preferred_element_type=jnp.float32,
            )
            dhidden = (dhidden * factor[span, columns]).astype(jnp.bfloat16)
            dpre[pl.ds(first, group), :, columns] = dhidden.reshape(group, cap, tile)

        each(0, ff // tile, pull)

    each(0, shifts, backward)

    def product(left, right, first, j, part):
        columns = pl.ds(pl.multiple_of(first + j * part, part), part)
        return lax.dot_general(
            left[:, :, columns].reshape(n * cap, part), right[...].reshape(n * cap, right.shape[2]),
            (((0,), (0,)), ((), ())), preferred_element_type=jnp.float32,
        )

    def gradient(left, right, give, came, result):
        half = give.shape[0]
        part = tile_of(half, 256)

        def theirs(j):
            give[pl.ds(pl.multiple_of(j * part, part), part), :] = product(
                left, right, other * half, j, part).astype(jnp.bfloat16)

        def mine(j):
            band = pl.ds(pl.multiple_of(j * part, part), part)
            result[band, :] = came[band, :].astype(jnp.float32) + product(left, right, core * half, j, part)

        return functools.partial(each, 0, half // part, theirs), functools.partial(each, 0, half // part, mine)

    theirs_out, mine_out = gradient(hidden, rows_g, give_out, came_out, grad_out)
    theirs_in, mine_in = gradient(rows_x, dpre, give_in, came_in, grad_in)
    theirs_out()
    pair_copy(0).start()
    theirs_in()
    pair_copy(1).start()
    pair_copy(0).wait_recv()
    mine_out()
    pair_copy(1).wait_recv()
    mine_in()
    pair_copy(0).wait_send()
    own_copy(2).wait()

    def merge(pieces, first, last):
        many = pieces[0][2] * cap
        lane = lax.broadcasted_iota(jnp.int32, (1, len(pieces) * many), 1)
        place = jnp.full(lane.shape, -1, jnp.int32)
        for at, (shift, low_turn, turns) in enumerate(pieces):
            inside = lane - at * many
            turn = lax.rem(inside // cap + low_turn + spot, group)
            found = (lax.rem(plane + shift, shifts) * group + turn) * cap + lax.rem(inside, cap)
            place = jnp.where((inside >= 0) & (inside < many), found, place)
        chosen = jnp.where(place == columns_of[:, 0:1].astype(jnp.int32), 1.0, 0.0).astype(jnp.bfloat16)
        for shift, low_turn, turns in pieces:
            def arrived(turn):
                @pl.when(shift * group + turn > 0)
                def _():
                    o_copy(shift, turn).wait_recv()

            each(low_turn, low_turn + turns, arrived)
        for j in range(width // wide):
            columns = pl.ds(j * wide, wide)
            block = jnp.concatenate([
                back[pl.ds(shift * group + low_turn, turns), :, columns].reshape(many, wide)
                for shift, low_turn, turns in pieces
            ], axis=0)
            added = jnp.dot(chosen, block, preferred_element_type=jnp.float32)
            if not first:
                added += total[:, columns]
            if last:
                mixed[:, columns] = (columns_of[:, 1:2] * added).astype(jnp.bfloat16)
            else:
                total[:, columns] = added

    far = [near_first(i, -1) for i in range(2, shifts)]
    half, quarter = group // 2, group // 4
    if shifts == 4 and quarter * 4 == group:
        merge([(0, 0, group)], True, False)
        merge([(near_first(1, -1), 0, group)], False, False)
        merge([(shift, 0, half) for shift in far], False, False)
        merge([(shift, half, quarter) for shift in far], False, False)
        final = [(shift, half + quarter, quarter) for shift in far]
    else:
        for shift in range(shifts - 1):
            merge([(shift, 0, group)], shift == 0, False)
        final = [(shifts - 1, 0, group)]

    def finish(shift, turn):
        x_copy(shift, turn).wait_send()
        g_copy(shift, turn).wait_send()

    each(0, shifts, lambda shift: blocks(shift, finish))
    pair_copy(1).wait_send()
    merge(final, shifts == 1, True)
    each(0, shifts, lambda shift: blocks(shift, lambda s, t: o_copy(s, t).wait_send()))


def exchange(n, cap, ids, prob, tokens, cotangent, keep, w_in, w_out):
    count, width = tokens.shape
    ff = w_in.shape[1]
    shifts = 4 if n % 4 == 0 else 1
    dma = pltpu.SemaphoreType.DMA
    f32, bf16 = jnp.float32, jnp.bfloat16
    whole = pl.BlockSpec(memory_space=pl.ANY)
    near = pl.BlockSpec(memory_space=pltpu.VMEM)
    flops = 10 * n * cap * width * ff
    return pl.pallas_call(
        functools.partial(kernel, n, shifts),
        out_shape=(
            pltpu.VMEM((count, width), bf16),
            pltpu.VMEM((width // 2, ff), f32),
            pltpu.VMEM((ff // 2, width), f32),
        ),
        in_specs=[whole] * 7,
        out_specs=(near, near, near),
        scratch_shapes=[
            pltpu.VMEM((1, count), jnp.int32),
            pltpu.VMEM((1, count), f32),
            pltpu.VMEM((count, width), bf16),
            pltpu.VMEM((count, width), bf16),
            pltpu.VMEM(keep.shape, jnp.int32),
            pltpu.VMEM((n, 1, ff), f32),
            pltpu.VMEM((1, count), jnp.int32),
            pltpu.VMEM((count, 128), f32),
            pltpu.VMEM((n, cap, width), bf16),
            pltpu.VMEM((n, cap, width), bf16),
            pltpu.VMEM((n, cap, width), bf16),
            pltpu.VMEM((width, ff), bf16),
            pltpu.VMEM((ff, width), bf16),
            pltpu.VMEM((n, cap, width), bf16),
            pltpu.VMEM((n, cap, width), bf16),
            pltpu.VMEM((n, cap, width), bf16),
            pltpu.VMEM((n, cap, ff), bf16),
            pltpu.VMEM((n * cap, ff), f32),
            pltpu.VMEM((n, cap, ff), bf16),
            pltpu.VMEM((ff // 2, width), bf16),
            pltpu.VMEM((width // 2, ff), bf16),
            pltpu.VMEM((ff // 2, width), bf16),
            pltpu.VMEM((width // 2, ff), bf16),
            dma((7,)), dma((3,)), dma((n,)), dma((n,)), dma((n,)), dma((n,)), dma((n,)), dma((n,)),
            dma((2,)), dma((2,)),
        ],
        cost_estimate=pl.CostEstimate(flops=flops, bytes_accessed=40 << 20, transcendentals=n * cap * ff),
        compiler_params=pltpu.CompilerParams(
            collective_id=0, has_side_effects=True, vmem_limit_bytes=52 << 20
        ),
    )(ids, prob, tokens, cotangent, keep, w_in, w_out)


def shards(tokens, expert_id, router_prob, keep_mask, w_in, w_out, cotangent):
    count = tokens.shape[0]
    n = lax.axis_size("expert")
    mixed, grad_in, grad_out = exchange(
        n, 2 * count // n, expert_id.reshape(1, count), router_prob.reshape(1, count),
        tokens, cotangent, keep_mask[0], w_in[0], w_out[0],
    )
    return (mixed, grad_in[None], grad_out[None])


def solution(mesh):
    in_specs = (
        P(("expert", "replica"), None),
        P(("expert", "replica"), None),
        P(("expert", "replica")),
        P("expert", None, None),
        P("expert", None, None),
        P("expert", None, None),
        P(("expert", "replica"), None),
    )
    out_specs = (
        P(("expert", "replica"), None),
        P("expert", "replica", None),
        P("expert", "replica", None),
    )
    return jax.shard_map(shards, mesh=mesh, in_specs=in_specs, out_specs=out_specs, check_vma=False)
```

```python
import functools

import jax
import jax.numpy as jnp
from jax import lax
from jax.experimental import pallas as pl
from jax.experimental.pallas import tpu as pltpu
from jax.sharding import PartitionSpec as P

KEEP_SCALE = 4.0 / 3.0
MESH = pl.DeviceIdType.MESH


def gelu_parts(pre):
    inner = 0.7978845608 * (pre + 0.044715 * pre * pre * pre)
    tanh_v = jnp.tanh(inner)
    value = 0.5 * pre * (1.0 + tanh_v)
    slope = 0.5 * (1.0 + tanh_v) + 0.5 * pre * (1.0 - tanh_v * tanh_v) * 0.7978845608 * (
        1.0 + 3.0 * 0.044715 * pre * pre
    )
    return (value, slope)


def tile_of(size, most):
    return size if size <= most else most


def each(low, high, step):
    def run(i, carry):
        step(i)
        return carry

    lax.fori_loop(low, high, run, 0)


def kernel(
    n, shifts,
    ids_in, prob_in, tokens, cotangent, keep, w_in, w_out,
    grad_in, grad_out, total, chosen_last, last_rows, columns_of,
    ids, prob, own_x, own_g, keep_raw, keep_rows, slot,
    sent, sent_grad, back,
    weight_in, weight_out, rows_x, rows_g, rows_o, hidden, factor, dpre,
    give_out, give_in, came_out, came_in,
    load_sem, own_sem, x_send, x_recv, g_send, g_recv, o_send, o_recv, pair_send, pair_recv,
):
    me = lax.axis_index("expert")
    core = lax.axis_index("replica")
    other = 1 - core
    group = n // shifts
    plane = me // group
    spot = lax.rem(me, group)
    cap, width = rows_x.shape[1:]
    ff = weight_in.shape[1]
    rows = group * cap
    tile = tile_of(ff, 512)
    wide = tile_of(width, 256)
    count = own_x.shape[0]

    def load(i):
        source, target = (
            (tokens, own_x), (cotangent, own_g), (keep, keep_raw), (w_in, weight_in), (w_out, weight_out),
            (ids_in, ids), (prob_in, prob),
        )[i]
        return pltpu.make_async_copy(source, target, load_sem.at[i])

    load(5).start()
    load(6).start()
    load(0).start()

    def ahead(shift, turn):
        return lax.rem(plane + shift, shifts) * group + lax.rem(spot + turn, group)

    def behind(shift, turn):
        return lax.rem(plane - shift + shifts, shifts) * group + lax.rem(spot - turn + group, group)

    def x_copy(shift, turn):
        k = shift * group + turn
        return pltpu.make_async_remote_copy(
            src_ref=sent.at[k], dst_ref=rows_x.at[k], send_sem=x_send.at[k],
            recv_sem=x_recv.at[k], device_id=(ahead(shift, turn), core), device_id_type=MESH,
        )

    def g_copy(shift, turn):
        k = shift * group + turn
        return pltpu.make_async_remote_copy(
            src_ref=sent_grad.at[k], dst_ref=rows_g.at[k], send_sem=g_send.at[k],
            recv_sem=g_recv.at[k], device_id=(ahead(shift, turn), core), device_id_type=MESH,
        )

    def o_copy(shift, turn):
        k = shift * group + turn
        return pltpu.make_async_remote_copy(
            src_ref=rows_o.at[k], dst_ref=back.at[k], send_sem=o_send.at[k],
            recv_sem=o_recv.at[k], device_id=(behind(shift, turn), core), device_id_type=MESH,
        )

    def own_copy(i):
        source, target = (
            (sent.at[0], rows_x.at[0]), (sent_grad.at[0], rows_g.at[0]), (rows_o.at[0], back.at[0])
        )[i]
        return pltpu.make_async_copy(source, target, own_sem.at[i])

    def pair_copy(i):
        source, target = ((give_out, came_out), (give_in, came_in))[i]
        return pltpu.make_async_remote_copy(
            src_ref=source, dst_ref=target, send_sem=pair_send.at[i],
            recv_sem=pair_recv.at[i], device_id=(me, other), device_id_type=MESH,
        )

    def blocks(shift, step):
        def one(turn):
            @pl.when(shift * group + turn > 0)
            def _():
                step(shift, turn)

        each(0, group, one)

    barrier = pltpu.get_barrier_semaphore()

    def greet(shift, turn):
        pl.semaphore_signal(barrier, inc=1, device_id=(ahead(shift, turn), core), device_id_type=MESH)

    each(0, shifts, lambda shift: blocks(shift, greet))
    pl.semaphore_signal(barrier, inc=1, device_id=(me, other), device_id_type=MESH)

    low = plane * 2 < shifts
    even = lax.rem(plane, 2) == 0

    def send_order(i):
        return jnp.where(low, lax.rem(i + 1, shifts), lax.rem(shifts - 1 - i + shifts, shifts))

    def near_first(i, sign):
        first = jnp.where(even, shifts - 1, 1)
        last = (plane + 3) // 2
        place = jnp.where(i == 0, 0, jnp.where(i == 1, first, jnp.where(i == 3, last, 6 - first - last)))
        if shifts != 4:
            place = i
        return place if sign > 0 else lax.rem(shifts - place, shifts)

    load(5).wait()
    load(6).wait()
    expert_rows = lax.broadcasted_iota(jnp.int32, (n, count), 0)
    hot = jnp.where(expert_rows == ids[...], 1.0, 0.0)
    before = lax.broadcasted_iota(jnp.int32, (count, count), 0) <= lax.broadcasted_iota(
        jnp.int32, (count, count), 1)
    counted = jnp.dot(
        hot.astype(jnp.bfloat16), jnp.where(before, 1.0, 0.0).astype(jnp.bfloat16),
        preferred_element_type=jnp.float32,
    )
    rank = jnp.sum(hot * counted, axis=0, keepdims=True) - 1.0
    place_of = ids[...] * cap + rank.astype(jnp.int32)
    slot[...] = place_of
    pair = lax.broadcasted_iota(jnp.int32, (128, count), 0) == 0
    columns_of[...] = jnp.transpose(jnp.where(pair, place_of.astype(jnp.float32), prob[...]))

    def dispatch(values, slots, shift):
        shape = (group, cap, count)
        turn = lax.broadcasted_iota(jnp.int32, shape, 0) + spot
        turn = jnp.where(turn >= group, turn - group, turn)
        place = (lax.rem(plane + shift, shifts) * group + turn) * cap + lax.broadcasted_iota(jnp.int32, shape, 1)
        chosen = jnp.where(place == slot[...][None], 1.0, 0.0).astype(jnp.bfloat16)
        filled = jnp.dot(
            chosen.reshape(rows, count), values[...], preferred_element_type=jnp.float32
        )
        slots[pl.ds(shift * group, group)] = filled.astype(jnp.bfloat16).reshape(group, cap, width)

    def start(copy):
        return lambda shift, turn: copy(shift, turn).start()

    load(0).wait()
    for i in range(1, 5):
        load(i).start()
    def send_x(i):
        dispatch(own_x, sent, send_order(i))

        @pl.when(i == 0)
        def _():
            pl.semaphore_wait(barrier, n)

        blocks(send_order(i), start(x_copy))

    each(0, shifts, send_x)
    own_copy(0).start()
    load(1).wait()
    own_g[...] = (columns_of[:, 1:2] * own_g[...].astype(jnp.float32)).astype(jnp.bfloat16)

    def send_g(i):
        dispatch(own_g, sent_grad, send_order(i))
        blocks(send_order(i), start(g_copy))

    each(0, shifts, send_g)
    own_copy(1).start()
    load(2).wait()

    def keep_row(k):
        source = behind(k // group, lax.rem(k, group)) * 2 + core
        keep_rows[k] = keep_raw[pl.ds(source, 1), :].astype(jnp.float32) * KEEP_SCALE

    each(0, n, keep_row)
    own_copy(0).wait()
    own_copy(1).wait()
    load(3).wait()
    load(4).wait()

    def forward(i):
        shift = near_first(i, 1)
        first = shift * group
        span = pl.ds(pl.multiple_of(first * cap, rows), rows)
        blocks(shift, lambda s, t: x_copy(s, t).wait_recv())

        def project(j):
            columns = pl.ds(pl.multiple_of(j * tile, tile), tile)
            block = rows_x[pl.ds(first, group)].reshape(rows, width)
            pre = jnp.dot(block, weight_in[:, columns], preferred_element_type=jnp.float32)
            value, slope = gelu_parts(pre)
            scale = keep_rows[pl.ds(first, group), :, columns]
            value = value.reshape(group, cap, tile) * scale
            slope = slope.reshape(group, cap, tile) * scale
            hidden[pl.ds(first, group), :, columns] = value.astype(jnp.bfloat16)
            factor[span, columns] = slope.reshape(rows, tile)

        each(0, ff // tile, project)

        def output(j):
            columns = pl.ds(pl.multiple_of(j * wide, wide), wide)
            block = hidden[pl.ds(first, group)].reshape(rows, ff)
            out = jnp.dot(block, weight_out[:, columns], preferred_element_type=jnp.float32)
            rows_o[pl.ds(first, group), :, columns] = out.astype(jnp.bfloat16).reshape(group, cap, wide)

        each(0, width // wide, output)

        @pl.when(i < shifts // 2)
        def _():
            blocks(shift, start(o_copy))

        @pl.when(shift == 0)
        def _():
            own_copy(2).start()

    each(0, shifts, forward)
    each(0, shifts - shifts // 2, lambda i: blocks(near_first(shifts - 1 - i, 1), start(o_copy)))

    def backward(i):
        shift = near_first(i, 1)
        first = shift * group
        span = pl.ds(pl.multiple_of(first * cap, rows), rows)
        blocks(shift, lambda s, t: g_copy(s, t).wait_recv())

        def pull(j):
            columns = pl.ds(pl.multiple_of(j * tile, tile), tile)
            block = rows_g[pl.ds(first, group)].reshape(rows, width)
            dhidden = lax.dot_general(
                block, weight_out[columns, :], (((1,), (1,)), ((), ())),
                preferred_element_type=jnp.float32,
            )
            dhidden = (dhidden * factor[span, columns]).astype(jnp.bfloat16)
            dpre[pl.ds(first, group), :, columns] = dhidden.reshape(group, cap, tile)

        each(0, ff // tile, pull)

    each(0, shifts, backward)

    def product(left, right, first, j, part):
        columns = pl.ds(pl.multiple_of(first + j * part, part), part)
        return lax.dot_general(
            left[:, :, columns].reshape(n * cap, part), right[...].reshape(n * cap, right.shape[2]),
            (((0,), (0,)), ((), ())), preferred_element_type=jnp.float32,
        )

    def gradient(left, right, give, came, result):
        half = give.shape[0]
        part = tile_of(half, 256)

        def theirs(j):
            give[pl.ds(pl.multiple_of(j * part, part), part), :] = product(
                left, right, other * half, j, part).astype(jnp.bfloat16)

        def mine(j):
            band = pl.ds(pl.multiple_of(j * part, part), part)
            result[band, :] = came[band, :].astype(jnp.float32) + product(left, right, core * half, j, part)

        return functools.partial(each, 0, half // part, theirs), functools.partial(each, 0, half // part, mine)

    theirs_out, mine_out = gradient(hidden, rows_g, give_out, came_out, grad_out)
    theirs_in, mine_in = gradient(rows_x, dpre, give_in, came_in, grad_in)
    theirs_out()
    pair_copy(0).start()
    theirs_in()
    pair_copy(1).start()
    pair_copy(0).wait_recv()
    mine_out()
    pair_copy(1).wait_recv()
    mine_in()
    pair_copy(0).wait_send()
    own_copy(2).wait()

    def merge(pieces, first, last):
        many = pieces[0][2] * cap
        lane = lax.broadcasted_iota(jnp.int32, (1, len(pieces) * many), 1)
        place = jnp.full(lane.shape, -1, jnp.int32)
        for at, (shift, low_turn, turns) in enumerate(pieces):
            inside = lane - at * many
            turn = lax.rem(inside // cap + low_turn + spot, group)
            found = (lax.rem(plane + shift, shifts) * group + turn) * cap + lax.rem(inside, cap)
            place = jnp.where((inside >= 0) & (inside < many), found, place)
        chosen = jnp.where(place == columns_of[:, 0:1].astype(jnp.int32), 1.0, 0.0).astype(jnp.bfloat16)
        if last:
            chosen_last[...] = chosen
            if first:
                total[...] = jnp.zeros_like(total)
        for shift, low_turn, turns in pieces:
            def arrived(turn):
                @pl.when(shift * group + turn > 0)
                def _():
                    o_copy(shift, turn).wait_recv()

            each(low_turn, low_turn + turns, arrived)
        if last:
            for at, (shift, low_turn, turns) in enumerate(pieces):
                last_rows[pl.ds(at * many, many), :] = back[
                    pl.ds(shift * group + low_turn, turns)].reshape(many, width)
            return
        for j in range(width // wide):
            columns = pl.ds(j * wide, wide)
            block = jnp.concatenate([
                back[pl.ds(shift * group + low_turn, turns), :, columns].reshape(many, wide)
                for shift, low_turn, turns in pieces
            ], axis=0)
            added = jnp.dot(chosen, block, preferred_element_type=jnp.float32)
            if not first:
                added += total[:, columns]
            total[:, columns] = added

    far = [near_first(i, -1) for i in range(2, shifts)]
    half, quarter = group // 2, group // 4
    if shifts == 4 and quarter * 4 == group:
        merge([(0, 0, group)], True, False)
        merge([(near_first(1, -1), 0, group)], False, False)
        merge([(shift, 0, half) for shift in far], False, False)
        merge([(shift, half, quarter) for shift in far], False, False)
        final = [(shift, half + quarter, quarter) for shift in far]
    else:
        for shift in range(shifts - 1):
            merge([(shift, 0, group)], shift == 0, False)
        final = [(shifts - 1, 0, group)]

    def finish(shift, turn):
        x_copy(shift, turn).wait_send()
        g_copy(shift, turn).wait_send()

    each(0, shifts, lambda shift: blocks(shift, finish))
    pair_copy(1).wait_send()
    merge(final, shifts == 1, True)
    each(0, shifts, lambda shift: blocks(shift, lambda s, t: o_copy(s, t).wait_send()))


def exchange(n, cap, ids, prob, tokens, cotangent, keep, w_in, w_out):
    count, width = tokens.shape
    ff = w_in.shape[1]
    shifts = 4 if n % 4 == 0 else 1
    last = n // 8 * cap if n % 16 == 0 else n // shifts * cap
    dma = pltpu.SemaphoreType.DMA
    f32, bf16 = jnp.float32, jnp.bfloat16
    whole = pl.BlockSpec(memory_space=pl.ANY)
    near = pl.BlockSpec(memory_space=pltpu.VMEM)
    flops = 10 * n * cap * width * ff
    return pl.pallas_call(
        functools.partial(kernel, n, shifts),
        out_shape=(
            pltpu.VMEM((width // 2, ff), f32),
            pltpu.VMEM((ff // 2, width), f32),
            pltpu.VMEM((count, width), f32),
            pltpu.VMEM((count, last), bf16),
            pltpu.VMEM((last, width), bf16),
            pltpu.VMEM((count, 128), f32),
        ),
        in_specs=[whole] * 7,
        out_specs=(near,) * 6,
        scratch_shapes=[
            pltpu.VMEM((1, count), jnp.int32),
            pltpu.VMEM((1, count), f32),
            pltpu.VMEM((count, width), bf16),
            pltpu.VMEM((count, width), bf16),
            pltpu.VMEM(keep.shape, jnp.int32),
            pltpu.VMEM((n, 1, ff), f32),
            pltpu.VMEM((1, count), jnp.int32),
            pltpu.VMEM((n, cap, width), bf16),
            pltpu.VMEM((n, cap, width), bf16),
            pltpu.VMEM((n, cap, width), bf16),
            pltpu.VMEM((width, ff), bf16),
            pltpu.VMEM((ff, width), bf16),
            pltpu.VMEM((n, cap, width), bf16),
            pltpu.VMEM((n, cap, width), bf16),
            pltpu.VMEM((n, cap, width), bf16),
            pltpu.VMEM((n, cap, ff), bf16),
            pltpu.VMEM((n * cap, ff), f32),
            pltpu.VMEM((n, cap, ff), bf16),
            pltpu.VMEM((ff // 2, width), bf16),
            pltpu.VMEM((width // 2, ff), bf16),
            pltpu.VMEM((ff // 2, width), bf16),
            pltpu.VMEM((width // 2, ff), bf16),
            dma((7,)), dma((3,)), dma((n,)), dma((n,)), dma((n,)), dma((n,)), dma((n,)), dma((n,)),
            dma((2,)), dma((2,)),
        ],
        cost_estimate=pl.CostEstimate(flops=flops, bytes_accessed=40 << 20, transcendentals=n * cap * ff),
        compiler_params=pltpu.CompilerParams(
            collective_id=0, has_side_effects=True, vmem_limit_bytes=50 << 20
        ),
    )(ids, prob, tokens, cotangent, keep, w_in, w_out)


def closing(
    sum_in, sum_out, total, chosen, rows, columns_of, mixed, grad_in, grad_out, held, sem
):
    copies = [
        pltpu.make_async_copy(source, target, sem.at[i])
        for i, (source, target) in enumerate(((sum_in, grad_in), (sum_out, grad_out), (held, mixed)))
    ]
    copies[0].start()
    copies[1].start()
    width = held.shape[1]
    wide = tile_of(width, 256)
    for j in range(width // wide):
        columns = pl.ds(j * wide, wide)
        added = total[:, columns] + jnp.dot(
            chosen[...], rows[:, columns], preferred_element_type=jnp.float32)
        held[:, columns] = (columns_of[:, 1:2] * added).astype(jnp.bfloat16)
    copies[2].start()
    for copy in copies:
        copy.wait()


def close(sum_in, sum_out, total, chosen, rows, columns_of):
    near = pl.BlockSpec(memory_space=pltpu.VMEM)
    whole = pl.BlockSpec(memory_space=pl.ANY)
    count, width = total.shape
    args = (sum_in, sum_out, total, chosen, rows, columns_of)
    return pl.pallas_call(
        closing,
        out_shape=(
            jax.ShapeDtypeStruct((count, width), jnp.bfloat16),
            jax.ShapeDtypeStruct(sum_in.shape, sum_in.dtype),
            jax.ShapeDtypeStruct(sum_out.shape, sum_out.dtype),
        ),
        in_specs=[near] * 6,
        out_specs=(whole, whole, whole),
        scratch_shapes=[pltpu.VMEM((count, width), jnp.bfloat16), pltpu.SemaphoreType.DMA((3,))],
        cost_estimate=pl.CostEstimate(
            flops=2 * chosen.size * width, bytes_accessed=9 << 20, transcendentals=0),
        compiler_params=pltpu.CompilerParams(vmem_limit_bytes=8 << 20),
    )(*[pltpu.with_memory_space_constraint(arg, pltpu.VMEM) for arg in args])


def shards(tokens, expert_id, router_prob, keep_mask, w_in, w_out, cotangent):
    count = tokens.shape[0]
    n = lax.axis_size("expert")
    mixed, grad_in, grad_out = close(*exchange(
        n, 2 * count // n, expert_id.reshape(1, count), router_prob.reshape(1, count),
        tokens, cotangent, keep_mask[0], w_in[0], w_out[0],
    ))
    return (mixed, grad_in[None], grad_out[None])


def solution(mesh):
    in_specs = (
        P(("expert", "replica"), None),
        P(("expert", "replica"), None),
        P(("expert", "replica")),
        P("expert", None, None),
        P("expert", None, None),
        P("expert", None, None),
        P(("expert", "replica"), None),
    )
    out_specs = (
        P(("expert", "replica"), None),
        P("expert", "replica", None),
        P("expert", "replica", None),
    )
    return jax.shard_map(shards, mesh=mesh, in_specs=in_specs, out_specs=out_specs, check_vma=False)
```

```python
import functools

import jax
import jax.numpy as jnp
from jax import lax
from jax.experimental import pallas as pl
from jax.experimental.pallas import tpu as pltpu
from jax.sharding import PartitionSpec as P

KEEP_SCALE = 4.0 / 3.0
MESH = pl.DeviceIdType.MESH


def gelu_parts(pre):
    inner = 0.7978845608 * (pre + 0.044715 * pre * pre * pre)
    tanh_v = jnp.tanh(inner)
    value = 0.5 * pre * (1.0 + tanh_v)
    slope = 0.5 * (1.0 + tanh_v) + 0.5 * pre * (1.0 - tanh_v * tanh_v) * 0.7978845608 * (
        1.0 + 3.0 * 0.044715 * pre * pre
    )
    return (value, slope)


def tile_of(size, most):
    return size if size <= most else most


def each(low, high, step):
    def run(i, carry):
        step(i)
        return carry

    lax.fori_loop(low, high, run, 0)


def kernel(
    n, shifts,
    ids_in, prob_in, tokens, cotangent, keep, w_in, w_out,
    grad_in, grad_out, total, chosen_last, last_rows, columns_of,
    ids, prob, own_x, own_g, keep_raw, keep_rows, slot,
    sent, sent_grad, back,
    weight_in, weight_out, rows_x, rows_g, rows_o, hidden, factor, dpre,
    give_out, give_in, came_out, came_in,
    load_sem, own_sem, x_send, x_recv, g_send, g_recv, o_send, o_recv, pair_send, pair_recv,
):
    me = lax.axis_index("expert")
    core = lax.axis_index("replica")
    other = 1 - core
    group = n // shifts
    plane = me // group
    spot = lax.rem(me, group)
    cap, width = rows_x.shape[1:]
    ff = weight_in.shape[1]
    rows = group * cap
    tile = tile_of(ff, 512)
    wide = tile_of(width, 256)
    count = own_x.shape[0]

    def load(i):
        source, target = (
            (tokens, own_x), (cotangent, own_g), (keep, keep_raw), (w_in, weight_in), (w_out, weight_out),
            (ids_in, ids), (prob_in, prob),
        )[i]
        return pltpu.make_async_copy(source, target, load_sem.at[i])

    load(5).start()
    load(6).start()
    load(0).start()

    def ahead(shift, turn):
        return lax.rem(plane + shift, shifts) * group + lax.rem(spot + turn, group)

    def behind(shift, turn):
        return lax.rem(plane - shift + shifts, shifts) * group + lax.rem(spot - turn + group, group)

    def x_copy(shift, turn):
        k = shift * group + turn
        return pltpu.make_async_remote_copy(
            src_ref=sent.at[k], dst_ref=rows_x.at[k], send_sem=x_send.at[k],
            recv_sem=x_recv.at[k], device_id=(ahead(shift, turn), core), device_id_type=MESH,
        )

    def g_copy(shift, turn):
        k = shift * group + turn
        return pltpu.make_async_remote_copy(
            src_ref=sent_grad.at[k], dst_ref=rows_g.at[k], send_sem=g_send.at[k],
            recv_sem=g_recv.at[k], device_id=(ahead(shift, turn), core), device_id_type=MESH,
        )

    def o_copy(shift, turn):
        k = shift * group + turn
        return pltpu.make_async_remote_copy(
            src_ref=rows_o.at[k], dst_ref=back.at[k], send_sem=o_send.at[k],
            recv_sem=o_recv.at[k], device_id=(behind(shift, turn), core), device_id_type=MESH,
        )

    def own_copy(i):
        source, target = (
            (sent.at[0], rows_x.at[0]), (sent_grad.at[0], rows_g.at[0]), (rows_o.at[0], back.at[0])
        )[i]
        return pltpu.make_async_copy(source, target, own_sem.at[i])

    def pair_copy(i):
        source, target = ((give_out, came_out), (give_in, came_in))[i]
        return pltpu.make_async_remote_copy(
            src_ref=source, dst_ref=target, send_sem=pair_send.at[i],
            recv_sem=pair_recv.at[i], device_id=(me, other), device_id_type=MESH,
        )

    def blocks(shift, step):
        def one(turn):
            @pl.when(shift * group + turn > 0)
            def _():
                step(shift, turn)

        each(0, group, one)

    barrier = pltpu.get_barrier_semaphore()

    def greet(shift, turn):
        pl.semaphore_signal(barrier, inc=1, device_id=(ahead(shift, turn), core), device_id_type=MESH)

    each(0, shifts, lambda shift: blocks(shift, greet))
    pl.semaphore_signal(barrier, inc=1, device_id=(me, other), device_id_type=MESH)

    low = plane * 2 < shifts
    even = lax.rem(plane, 2) == 0

    def send_order(i):
        return jnp.where(low, lax.rem(i + 1, shifts), lax.rem(shifts - 1 - i + shifts, shifts))

    def near_first(i, sign):
        first = jnp.where(even, shifts - 1, 1)
        last = (plane + 3) // 2
        place = jnp.where(i == 0, 0, jnp.where(i == 1, first, jnp.where(i == 3, last, 6 - first - last)))
        if shifts != 4:
            place = i
        return place if sign > 0 else lax.rem(shifts - place, shifts)

    load(5).wait()
    load(6).wait()
    expert_rows = lax.broadcasted_iota(jnp.int32, (n, count), 0)
    hot = jnp.where(expert_rows == ids[...], 1.0, 0.0)
    before = lax.broadcasted_iota(jnp.int32, (count, count), 0) <= lax.broadcasted_iota(
        jnp.int32, (count, count), 1)
    counted = jnp.dot(
        hot.astype(jnp.bfloat16), jnp.where(before, 1.0, 0.0).astype(jnp.bfloat16),
        preferred_element_type=jnp.float32,
    )
    rank = jnp.sum(hot * counted, axis=0, keepdims=True) - 1.0
    place_of = ids[...] * cap + rank.astype(jnp.int32)
    slot[...] = place_of
    pair = lax.broadcasted_iota(jnp.int32, (128, count), 0) == 0
    columns_of[...] = jnp.transpose(jnp.where(pair, place_of.astype(jnp.float32), prob[...]))

    def dispatch(values, slots, shift):
        shape = (group, cap, count)
        turn = lax.broadcasted_iota(jnp.int32, shape, 0) + spot
        turn = jnp.where(turn >= group, turn - group, turn)
        place = (lax.rem(plane + shift, shifts) * group + turn) * cap + lax.broadcasted_iota(jnp.int32, shape, 1)
        chosen = jnp.where(place == slot[...][None], 1.0, 0.0).astype(jnp.bfloat16)
        filled = jnp.dot(
            chosen.reshape(rows, count), values[...], preferred_element_type=jnp.float32
        )
        slots[pl.ds(shift * group, group)] = filled.astype(jnp.bfloat16).reshape(group, cap, width)

    def start(copy):
        return lambda shift, turn: copy(shift, turn).start()

    load(0).wait()
    for i in range(1, 5):
        load(i).start()
    def turned(shift, step):
        def one(i):
            turn = lax.rem(i + core * (group // 2), group)

            @pl.when(shift * group + turn > 0)
            def _():
                step(shift, turn)

        each(0, group, one)

    def send_x(i):
        dispatch(own_x, sent, send_order(i))

        @pl.when(i == 0)
        def _():
            pl.semaphore_wait(barrier, n)

        turned(send_order(i), start(x_copy))

    each(0, shifts, send_x)
    own_copy(0).start()
    load(1).wait()
    own_g[...] = (columns_of[:, 1:2] * own_g[...].astype(jnp.float32)).astype(jnp.bfloat16)

    def send_g(i):
        dispatch(own_g, sent_grad, send_order(i))
        turned(send_order(i), start(g_copy))

    each(0, shifts, send_g)
    own_copy(1).start()
    load(2).wait()

    def keep_row(k):
        source = behind(k // group, lax.rem(k, group)) * 2 + core
        keep_rows[k] = keep_raw[pl.ds(source, 1), :].astype(jnp.float32) * KEEP_SCALE

    each(0, n, keep_row)
    own_copy(0).wait()
    own_copy(1).wait()
    load(3).wait()
    load(4).wait()

    def forward(i):
        shift = near_first(i, 1)
        first = shift * group
        span = pl.ds(pl.multiple_of(first * cap, rows), rows)
        blocks(shift, lambda s, t: x_copy(s, t).wait_recv())

        def project(j):
            columns = pl.ds(pl.multiple_of(j * tile, tile), tile)
            block = rows_x[pl.ds(first, group)].reshape(rows, width)
            pre = jnp.dot(block, weight_in[:, columns], preferred_element_type=jnp.float32)
            value, slope = gelu_parts(pre)
            scale = keep_rows[pl.ds(first, group), :, columns]
            value = value.reshape(group, cap, tile) * scale
            slope = slope.reshape(group, cap, tile) * scale
            hidden[pl.ds(first, group), :, columns] = value.astype(jnp.bfloat16)
            factor[span, columns] = slope.reshape(rows, tile)

        each(0, ff // tile, project)

        def output(j):
            columns = pl.ds(pl.multiple_of(j * wide, wide), wide)
            block = hidden[pl.ds(first, group)].reshape(rows, ff)
            out = jnp.dot(block, weight_out[:, columns], preferred_element_type=jnp.float32)
            rows_o[pl.ds(first, group), :, columns] = out.astype(jnp.bfloat16).reshape(group, cap, wide)

        each(0, width // wide, output)

        @pl.when(i < shifts // 2)
        def _():
            blocks(shift, start(o_copy))

        @pl.when(shift == 0)
        def _():
            own_copy(2).start()

    each(0, shifts, forward)
    each(0, shifts - shifts // 2, lambda i: turned(near_first(shifts - 1 - i, 1), start(o_copy)))

    def backward(i):
        shift = near_first(i, 1)
        first = shift * group
        span = pl.ds(pl.multiple_of(first * cap, rows), rows)
        blocks(shift, lambda s, t: g_copy(s, t).wait_recv())

        def pull(j):
            columns = pl.ds(pl.multiple_of(j * tile, tile), tile)
            block = rows_g[pl.ds(first, group)].reshape(rows, width)
            dhidden = lax.dot_general(
                block, weight_out[columns, :], (((1,), (1,)), ((), ())),
                preferred_element_type=jnp.float32,
            )
            dhidden = (dhidden * factor[span, columns]).astype(jnp.bfloat16)
            dpre[pl.ds(first, group), :, columns] = dhidden.reshape(group, cap, tile)

        each(0, ff // tile, pull)

    each(0, shifts, backward)

    def product(left, right, first, j, part):
        columns = pl.ds(pl.multiple_of(first + j * part, part), part)
        return lax.dot_general(
            left[:, :, columns].reshape(n * cap, part), right[...].reshape(n * cap, right.shape[2]),
            (((0,), (0,)), ((), ())), preferred_element_type=jnp.float32,
        )

    def gradient(left, right, give, came, result):
        half = give.shape[0]
        part = tile_of(half, 256)

        def theirs(j):
            give[pl.ds(pl.multiple_of(j * part, part), part), :] = product(
                left, right, other * half, j, part).astype(jnp.bfloat16)

        def mine(j):
            band = pl.ds(pl.multiple_of(j * part, part), part)
            result[band, :] = came[band, :].astype(jnp.float32) + product(left, right, core * half, j, part)

        return functools.partial(each, 0, half // part, theirs), functools.partial(each, 0, half // part, mine)

    theirs_out, mine_out = gradient(hidden, rows_g, give_out, came_out, grad_out)
    theirs_in, mine_in = gradient(rows_x, dpre, give_in, came_in, grad_in)
    theirs_out()
    pair_copy(0).start()
    theirs_in()
    pair_copy(1).start()
    pair_copy(0).wait_recv()
    mine_out()
    pair_copy(1).wait_recv()
    mine_in()
    pair_copy(0).wait_send()
    own_copy(2).wait()

    def merge(pieces, first, last):
        many = pieces[0][2] * cap
        lane = lax.broadcasted_iota(jnp.int32, (1, len(pieces) * many), 1)
        place = jnp.full(lane.shape, -1, jnp.int32)
        for at, (shift, low_turn, turns) in enumerate(pieces):
            inside = lane - at * many
            turn = lax.rem(inside // cap + low_turn + spot, group)
            found = (lax.rem(plane + shift, shifts) * group + turn) * cap + lax.rem(inside, cap)
            place = jnp.where((inside >= 0) & (inside < many), found, place)
        chosen = jnp.where(place == columns_of[:, 0:1].astype(jnp.int32), 1.0, 0.0).astype(jnp.bfloat16)
        if last:
            chosen_last[...] = chosen
            if first:
                total[...] = jnp.zeros_like(total)
        for shift, low_turn, turns in pieces:
            def arrived(turn):
                @pl.when(shift * group + turn > 0)
                def _():
                    o_copy(shift, turn).wait_recv()

            each(low_turn, low_turn + turns, arrived)
        if last:
            for at, (shift, low_turn, turns) in enumerate(pieces):
                last_rows[pl.ds(at * many, many), :] = back[
                    pl.ds(shift * group + low_turn, turns)].reshape(many, width)
            return
        for j in range(width // wide):
            columns = pl.ds(j * wide, wide)
            block = jnp.concatenate([
                back[pl.ds(shift * group + low_turn, turns), :, columns].reshape(many, wide)
                for shift, low_turn, turns in pieces
            ], axis=0)
            added = jnp.dot(chosen, block, preferred_element_type=jnp.float32)
            if not first:
                added += total[:, columns]
            total[:, columns] = added

    far = [near_first(i, -1) for i in range(2, shifts)]
    half, quarter = group // 2, group // 4
    if shifts == 4 and quarter * 4 == group:
        merge([(0, 0, group)], True, False)
        merge([(near_first(1, -1), 0, group)], False, False)
        begin = core * half
        merge([(shift, begin, half) for shift in far], False, False)
        begin = lax.rem(begin + half, group)
        merge([(shift, begin, quarter) for shift in far], False, False)
        final = [(shift, begin + quarter, quarter) for shift in far]
    else:
        for shift in range(shifts - 1):
            merge([(shift, 0, group)], shift == 0, False)
        final = [(shifts - 1, 0, group)]

    def finish(shift, turn):
        x_copy(shift, turn).wait_send()
        g_copy(shift, turn).wait_send()

    each(0, shifts, lambda shift: blocks(shift, finish))
    pair_copy(1).wait_send()
    merge(final, shifts == 1, True)
    each(0, shifts, lambda shift: blocks(shift, lambda s, t: o_copy(s, t).wait_send()))


def exchange(n, cap, ids, prob, tokens, cotangent, keep, w_in, w_out):
    count, width = tokens.shape
    ff = w_in.shape[1]
    shifts = 4 if n % 4 == 0 else 1
    last = n // 8 * cap if n % 16 == 0 else n // shifts * cap
    dma = pltpu.SemaphoreType.DMA
    f32, bf16 = jnp.float32, jnp.bfloat16
    whole = pl.BlockSpec(memory_space=pl.ANY)
    near = pl.BlockSpec(memory_space=pltpu.VMEM)
    flops = 10 * n * cap * width * ff
    return pl.pallas_call(
        functools.partial(kernel, n, shifts),
        out_shape=(
            pltpu.VMEM((width // 2, ff), f32),
            pltpu.VMEM((ff // 2, width), f32),
            pltpu.VMEM((count, width), f32),
            pltpu.VMEM((count, last), bf16),
            pltpu.VMEM((last, width), bf16),
            pltpu.VMEM((count, 128), f32),
        ),
        in_specs=[whole] * 7,
        out_specs=(near,) * 6,
        scratch_shapes=[
            pltpu.VMEM((1, count), jnp.int32),
            pltpu.VMEM((1, count), f32),
            pltpu.VMEM((count, width), bf16),
            pltpu.VMEM((count, width), bf16),
            pltpu.VMEM(keep.shape, jnp.int32),
            pltpu.VMEM((n, 1, ff), f32),
            pltpu.VMEM((1, count), jnp.int32),
            pltpu.VMEM((n, cap, width), bf16),
            pltpu.VMEM((n, cap, width), bf16),
            pltpu.VMEM((n, cap, width), bf16),
            pltpu.VMEM((width, ff), bf16),
            pltpu.VMEM((ff, width), bf16),
            pltpu.VMEM((n, cap, width), bf16),
            pltpu.VMEM((n, cap, width), bf16),
            pltpu.VMEM((n, cap, width), bf16),
            pltpu.VMEM((n, cap, ff), bf16),
            pltpu.VMEM((n * cap, ff), f32),
            pltpu.VMEM((n, cap, ff), bf16),
            pltpu.VMEM((ff // 2, width), bf16),
            pltpu.VMEM((width // 2, ff), bf16),
            pltpu.VMEM((ff // 2, width), bf16),
            pltpu.VMEM((width // 2, ff), bf16),
            dma((7,)), dma((3,)), dma((n,)), dma((n,)), dma((n,)), dma((n,)), dma((n,)), dma((n,)),
            dma((2,)), dma((2,)),
        ],
        cost_estimate=pl.CostEstimate(flops=flops, bytes_accessed=40 << 20, transcendentals=n * cap * ff),
        compiler_params=pltpu.CompilerParams(
            collective_id=0, has_side_effects=True, vmem_limit_bytes=50 << 20
        ),
    )(ids, prob, tokens, cotangent, keep, w_in, w_out)


def closing(
    sum_in, sum_out, total, chosen, rows, columns_of, mixed, grad_in, grad_out, held, sem
):
    copies = [
        pltpu.make_async_copy(source, target, sem.at[i])
        for i, (source, target) in enumerate(((sum_in, grad_in), (sum_out, grad_out), (held, mixed)))
    ]
    copies[0].start()
    copies[1].start()
    width = held.shape[1]
    wide = tile_of(width, 256)
    for j in range(width // wide):
        columns = pl.ds(j * wide, wide)
        added = total[:, columns] + jnp.dot(
            chosen[...], rows[:, columns], preferred_element_type=jnp.float32)
        held[:, columns] = (columns_of[:, 1:2] * added).astype(jnp.bfloat16)
    copies[2].start()
    for copy in copies:
        copy.wait()


def close(sum_in, sum_out, total, chosen, rows, columns_of):
    near = pl.BlockSpec(memory_space=pltpu.VMEM)
    whole = pl.BlockSpec(memory_space=pl.ANY)
    count, width = total.shape
    args = (sum_in, sum_out, total, chosen, rows, columns_of)
    return pl.pallas_call(
        closing,
        out_shape=(
            jax.ShapeDtypeStruct((count, width), jnp.bfloat16),
            jax.ShapeDtypeStruct(sum_in.shape, sum_in.dtype),
            jax.ShapeDtypeStruct(sum_out.shape, sum_out.dtype),
        ),
        in_specs=[near] * 6,
        out_specs=(whole, whole, whole),
        scratch_shapes=[pltpu.VMEM((count, width), jnp.bfloat16), pltpu.SemaphoreType.DMA((3,))],
        cost_estimate=pl.CostEstimate(
            flops=2 * chosen.size * width, bytes_accessed=9 << 20, transcendentals=0),
        compiler_params=pltpu.CompilerParams(vmem_limit_bytes=8 << 20),
    )(*[pltpu.with_memory_space_constraint(arg, pltpu.VMEM) for arg in args])


def shards(tokens, expert_id, router_prob, keep_mask, w_in, w_out, cotangent):
    count = tokens.shape[0]
    n = lax.axis_size("expert")
    mixed, grad_in, grad_out = close(*exchange(
        n, 2 * count // n, expert_id.reshape(1, count), router_prob.reshape(1, count),
        tokens, cotangent, keep_mask[0], w_in[0], w_out[0],
    ))
    return (mixed, grad_in[None], grad_out[None])


def solution(mesh):
    in_specs = (
        P(("expert", "replica"), None),
        P(("expert", "replica"), None),
        P(("expert", "replica")),
        P("expert", None, None),
        P("expert", None, None),
        P("expert", None, None),
        P(("expert", "replica"), None),
    )
    out_specs = (
        P(("expert", "replica"), None),
        P("expert", "replica", None),
        P("expert", "replica", None),
    )
    return jax.shard_map(shards, mesh=mesh, in_specs=in_specs, out_specs=out_specs, check_vma=False)
```
